16 devices in a mesh: rep: 2 (over y, z), dp: 8 (over x, core).
Axes of the slice: x: 4, y: 2, z: 1, core: 2. Of those that a mesh axis runs over, the one named last changes fastest.
The devices are a block of a 4x4x8 slice.
Arguments:
- x: bfloat16 [16, 2048, 1024], P(('rep', 'dp')), parts along dimension 0
- dy: bfloat16 [16, 2048, 1024], P(('rep', 'dp')), parts along dimension 0
- w_gate: bfloat16 [2, 1024, 3072], P(None, 'dp')
- w_up: bfloat16 [2, 1024, 3072], P(None, 'dp')
- w_down: bfloat16 [2, 3072, 1024], P(None, 'dp')
- m_w_gate: float32 [2, 1024, 3072], P(None, 'dp')
- m_w_up: float32 [2, 1024, 3072], P(None, 'dp')
- m_w_down: float32 [2, 3072, 1024], P(None, 'dp')
- v_w_gate: float32 [2, 1024, 3072], P(None, 'dp')
- v_w_up: float32 [2, 1024, 3072], P(None, 'dp')
- v_w_down: float32 [2, 3072, 1024], P(None, 'dp')
Outputs:
- output 1: bfloat16 [4, 1024, 3072], P('rep', 'dp'), parts along dimension 0
- output 2: bfloat16 [4, 1024, 3072], P('rep', 'dp'), parts along dimension 0
- output 3: bfloat16 [4, 3072, 1024], P('rep', 'dp'), parts along dimension 0
- output 4: float32 [4, 1024, 3072], P('rep', 'dp'), parts along dimension 0
- output 5: float32 [4, 1024, 3072], P('rep', 'dp'), parts along dimension 0
- output 6: float32 [4, 3072, 1024], P('rep', 'dp'), parts along dimension 0
- output 7: float32 [4, 1024, 3072], P('rep', 'dp'), parts along dimension 0
- output 8: float32 [4, 1024, 3072], P('rep', 'dp'), parts along dimension 0
- output 9: float32 [4, 3072, 1024], P('rep', 'dp'), parts along dimension 0
There are 2 independent parts. The reference program is written for one: setup_inputs(seed, part) draws one part's arguments, and reference() takes and returns one part's arrays. A program takes and returns all parts, laid end to end along the dimension named above; an argument that names none is the same for every part.
All inputs are finite; a program needn't handle non-finite values.
Results may differ from the reference program's by a relative error of at most 0.022.
Values are sent between devices in bfloat16 or wider.
A program may use at most 768 MiB of HBM per device.

```python
import jax
import jax.numpy as jnp
from jax import lax

SEQUENCES = 8
TOKENS = 2048
D = 1024
FF = 3072
LAYERS = 2
NAMES = ("w_gate", "w_up", "w_down")
SHAPES = {"w_gate": (LAYERS, D, FF), "w_up": (LAYERS, D, FF), "w_down": (LAYERS, FF, D)}


def bump(key, n, height):
    away = (jnp.arange(n, dtype=jnp.int32) - jax.random.randint(key, (), 0, n, jnp.int32)) % n
    return jnp.where(away < n // 8, height, 1.0)


def together(key, own, strength):
    shared = jax.random.normal(key, own.shape[1:], jnp.float32)
    return (own + strength * shared) * lax.rsqrt(1 + strength * strength)


def setup_inputs(seed: int = 0, part: int = 0) -> dict:
    kx, kdy, ka, kb, kz, kf, kh, kl, *keys = jax.random.split(jax.random.key(seed), 8 + 3 * len(NAMES))
    kx, kdy, ka, kb = (jax.random.fold_in(k, part) for k in (kx, kdy, ka, kb))
    kw, km, kv = (keys[i::3] for i in range(3))
    shape = (SEQUENCES, TOKENS, D)
    much_x, much_dy = jax.random.uniform(kz, (2,), jnp.float32, 0.0, 1.0)
    loud = 2.0 ** jax.random.uniform(jax.random.fold_in(kz, 1), (), jnp.float32, -1.0, 2.0)
    layers = 2.0 ** jax.random.uniform(kl, (LAYERS, 1, 1), jnp.float32, -1.0, 1.0)
    x = together(ka, jax.random.normal(kx, shape, jnp.float32), much_x) * bump(kf, D, 4.0)
    dy = together(kb, jax.random.normal(kdy, shape, jnp.float32), much_dy)
    drawn = {"x": x.astype(jnp.bfloat16), "dy": (loud * dy * (SEQUENCES * TOKENS) ** -0.5).astype(jnp.bfloat16)}
    for key, name in zip(kw, NAMES, strict=True):
        w = jax.random.normal(key, SHAPES[name], jnp.float32) * SHAPES[name][1] ** -0.5
        drawn[name] = (w * {"w_gate": 1.0, "w_up": bump(kh, FF, 4.0), "w_down": layers}[name]).astype(jnp.bfloat16)
    for key, name in zip(km, NAMES, strict=True):
        drawn[f"m_{name}"] = 0.1 * jax.random.normal(key, SHAPES[name], jnp.float32)
    for key, name in zip(kv, NAMES, strict=True):
        drawn[f"v_{name}"] = jax.random.uniform(key, SHAPES[name], jnp.float32, 0.005, 0.015)
    return drawn


def matmul(a, w):
    return jnp.dot(a, w, preferred_element_type=jnp.float32).astype(jnp.bfloat16)


def normed(h):
    wide = h.astype(jnp.float32)
    scale = lax.rsqrt(jnp.mean(wide**2, -1, keepdims=True) + 1e-6)
    return (wide * scale).astype(jnp.bfloat16)


def layer(h, w):
    a = normed(h)
    gate = jnp.dot(a, w["w_gate"], preferred_element_type=jnp.float32)
    up = jnp.dot(a, w["w_up"], preferred_element_type=jnp.float32)
    return h + matmul((jax.nn.silu(gate) * up).astype(jnp.bfloat16), w["w_down"])


def adamw(w, m, v, g):
    m = 0.9 * m + 0.1 * g
    v = 0.95 * v + 0.05 * g * g
    step = m * lax.rsqrt(v + 1e-8) + 0.1 * w
    return (w - 0.02 * step).astype(jnp.bfloat16), m, v


def clipped(gradients, sum_of_squares, count):
    factor = jnp.minimum(1.0, 0.5 * lax.rsqrt(sum_of_squares / count + 1e-30))
    return [g * factor for g in gradients]


def stack(weights, h):
    return lax.scan(lambda h, w: (layer(h, w), None), h, weights)[0]


def reference(x, dy, w_gate, w_up, w_down, m_w_gate, m_w_up, m_w_down, v_w_gate, v_w_up, v_w_down):
    weights = dict(zip(NAMES, (w_gate, w_up, w_down), strict=True))

    def take(so_far, sequence):
        h, by_y = sequence
        _, back = jax.vjp(lambda w: stack(w, h), weights)
        return jax.tree.map(lambda total, term: total + term.astype(jnp.float32), so_far, back(by_y)[0]), None

    none_yet = {name: jnp.zeros(w.shape, jnp.float32) for name, w in weights.items()}
    by_weights, _ = lax.scan(take, none_yet, (x, dy))
    gradients = [by_weights[name].astype(jnp.bfloat16).astype(jnp.float32) for name in NAMES]
    gradients = clipped(gradients, sum(jnp.sum(g * g) for g in gradients), sum(g.size for g in gradients))
    new = [
        adamw(w.astype(jnp.float32), m, v, g)
        for w, m, v, g in zip((w_gate, w_up, w_down), (m_w_gate, m_w_up, m_w_down), (v_w_gate, v_w_up, v_w_down), gradients, strict=True)
    ]
    return tuple(one[which] for which in range(3) for one in new)
```

```python
import functools

import jax
import jax.numpy as jnp
from jax import lax
from jax.experimental import pallas as pl
from jax.experimental.pallas import tpu as pltpu
from jax.sharding import PartitionSpec as P

F32, BF16 = jnp.float32, jnp.bfloat16
MESH = pl.DeviceIdType.MESH
LANES = 128
TILE = 256
SLOTS = 6
NT = (((1,), (1,)), ((), ()))


def dot(a, b):
    return jnp.dot(a, b, preferred_element_type=F32)


def dot_nt(a, b):
    return lax.dot_general(a, b, NT, preferred_element_type=F32)


def loop(lo, hi, body):
    lax.fori_loop(lo, hi, lambda i, _: (body(i), None)[1], None)


def when(cond):
    return pl.when(cond)


def step_kernel(
    x_ref, dy_ref, wg_ref, wu_ref, wd_ref,
    gg_ref, gd_ref, ssq_ref, gu0_ref, p0_ref, h1_ref, a0t_ref, wd0_ref,
    a, at, dyb, dyt, acc, pbuf, gsl, wdr, dto, own, prt, st1, st2, r1, r2, gout, stg, sq, sqall,
    sem_in, sem_stg, sem_p, sem_h, sem_out, sem_own, sem_wd, sem_stash,
    ag_send, ag_recv, dg_send, dg_recv, r0_send, r0_recv, r1_send, r1_recv, r2_send, r2_recv, sq_send, sq_recv,
    *, n,
):
    chips = n // 2
    tokens, d = a.shape
    tiles = chips * 3
    mb, mf = tokens // 2, tokens // 4
    rb = tokens // 4
    me = lax.axis_index("dp")
    i, c = me // 2, me % 2
    ir, il, io = (i + 1) % chips, (i + chips - 1) % chips, (i + 2) % chips
    right, left, opp, partner = 2 * ir + c, 2 * il + c, 2 * io + c, 2 * i + (1 - c)

    def remote(src, dst, send, recv, to):
        return pltpu.make_async_remote_copy(src, dst, send, recv, device_id={"dp": to}, device_id_type=MESH)

    def in_copy(k, which):
        rows = pl.ds(k * rb, rb)
        return pltpu.make_async_copy((x_ref, dy_ref)[which].at[0, rows], (a, dyb)[which].at[rows], sem_in.at[which, k])

    for k in range(4):
        in_copy(k, 0).start()
        in_copy(k, 1).start()

    def has_gu(x):
        return ((x >= 0) & (x < tiles)) | ((x >= tiles + 4) & (x < 2 * tiles + 4))

    def gidx(x):
        return jnp.where(x < tiles, x, x - 4)

    def has_d(x):
        return (x >= 0) & (x < 2 * tiles)

    def gu_view(x, dev, half=None):
        s = lax.rem(gidx(x), SLOTS)
        if half is None:
            return gsl.at[s, dev]
        return gsl.at[s, dev, pl.ds(2 * half, 2)]

    def d_view(x, dev, half=None):
        s, k = lax.rem(x // 4, 3), lax.rem(x, 4)
        cols = pl.ds(pl.multiple_of(k * 256, 256), 256)
        if half is None:
            return wdr.at[s, dev, :, cols]
        return wdr.at[s, dev, pl.ds(64 * half, 64), cols]

    streams = (
        (has_gu, gu_view, ag_send, ag_recv, lambda x: lax.rem(gidx(x), SLOTS)),
        (has_d, d_view, dg_send, dg_recv, lambda x: lax.rem(x, SLOTS)),
    )

    def own_gu(x):
        g = gidx(x)
        layer, t = g // tiles, lax.rem(g, tiles)
        ch, q = t // 4, lax.rem(t, 4)
        s = lax.rem(g, SLOTS)
        out = []
        for b in range(4):
            col = pl.multiple_of(LANES * (6 * q + 3 * (b % 2) + ch), LANES)
            src = (wg_ref, wu_ref)[b // 2].at[layer, :, pl.ds(col, LANES)]
            out.append(pltpu.make_async_copy(src, gsl.at[s, me, b], sem_own.at[lax.rem(g, 2)]))
        return out

    def own_gu_wait(x):
        g = gidx(x)
        whole = gsl.at[lax.rem(g, SLOTS), me]
        pltpu.make_async_copy(whole, whole, sem_own.at[lax.rem(g, 2)]).wait()

    def own_d(chunk):
        layer, ch = chunk // 3, lax.rem(chunk, 3)
        return pltpu.make_async_copy(wd_ref.at[layer, pl.ds(pl.multiple_of(LANES * ch, LANES), LANES)], wdr.at[ch, me], sem_wd.at[ch])

    def stash(chunk):
        return pltpu.make_async_copy(wdr.at[chunk], wd0_ref.at[chunk], sem_stash)

    def ag_copies(view, send, recv, s, x):
        def cp(name_s, name_r, dev, to, half=None):
            v = view(x, dev, half)
            return remote(v, v, send.at[name_s, s], recv.at[name_r, s], to)
        return dict(
            own_r=lambda: cp(0, 0, me, right), own_l=lambda: cp(1, 1, me, left), own_p=lambda: cp(2, 2, me, partner),
            l_p=lambda: cp(3, 3, left, partner), l_r=lambda: cp(4, 4, left, right, 0),
            r_p=lambda: cp(5, 5, right, partner), r_l=lambda: cp(6, 6, right, left, 1),
            o_p=lambda: cp(7, 7, opp, partner),
        )

    def got(view, recv, send, s, x, name, dev, half=None):
        v = view(x, dev, half)
        remote(v, v, send.at[name, s], recv.at[name, s], partner).wait_recv()

    def other(dev):
        return dev + 1 - 2 * lax.rem(dev, 2)

    def ag_step(t):
        @when(has_gu(t + 4))
        def _():
            for cp in own_gu(t + 4):
                cp.start()

        x4 = t + 4
        @when(has_d(x4) & (lax.rem(x4, 4) == 0) & (x4 >= tiles))
        def _():
            own_d(x4 // 4).start()

        for has, view, send, recv, sl in streams:
            x = t + 3
            @when(has(x))
            def _():
                if view is gu_view:
                    own_gu_wait(x)
                else:
                    @when(lax.rem(x, 4) == 0)
                    def _():
                        own_d(x // 4).wait()
                k = ag_copies(view, send, recv, sl(x), x)
                k["own_r"]().start()
                k["own_l"]().start()
                k["own_p"]().start()
        for has, view, send, recv, sl in streams:
            y = t + 2
            @when(has(y))
            def _():
                s = sl(y)
                k = ag_copies(view, send, recv, s, y)
                got(view, recv, send, s, y, 0, left)
                k["l_r"]().start()
                k["l_p"]().start()
                got(view, recv, send, s, y, 1, right)
                k["r_l"]().start()
                k["r_p"]().start()
        for has, view, send, recv, sl in streams:
            z = t + 1
            @when(has(z))
            def _():
                s = sl(z)
                got(view, recv, send, s, z, 4, opp, 0)
                got(view, recv, send, s, z, 6, opp, 1)
                ag_copies(view, send, recv, s, z)["o_p"]().start()
        for has, view, send, recv, sl in streams:
            @when(has(t))
            def _():
                s = sl(t)
                got(view, recv, send, s, t, 2, partner)
                got(view, recv, send, s, t, 3, other(left))
                got(view, recv, send, s, t, 5, other(right))
                got(view, recv, send, s, t, 7, other(opp))
                for make in ag_copies(view, send, recv, s, t).values():
                    make().wait_send()

    steps = 2 * tiles + 4
    half_d, full_d, full_gu = LANES, 2 * LANES, 4 * LANES

    def has_rs_gu(r):
        return ((r >= 0) & (r < tiles)) | ((r >= tiles + 4) & (r < steps))

    def has_rs_d(r):
        return (r >= 4) & (r < steps)

    parts = ((has_rs_gu, 0, 0, full_gu), (has_rs_d, 1, full_gu, full_d))

    def total(r, j, rows):
        return own[lax.rem(r, 4), c, j, rows].astype(F32) + prt[lax.rem(r, 5), j, rows].astype(F32)

    def blocks(lo, first, count, body):
        loop(first, first + count, lambda b: body(pl.ds(pl.multiple_of(lo + b * LANES, LANES), LANES)))

    def rs_cores(part, r):
        _, w, lo, size = part
        s = lax.rem(r, 5)
        rows = pl.ds(lo, size)
        return remote(own.at[lax.rem(r, 4), 1 - c, :, rows], prt.at[s, :, rows], r0_send.at[w, s], r0_recv.at[w, s], partner)

    def rs_far(part, r, side):
        _, w, lo, size = part
        s = lax.rem(r, 2)
        rows = pl.ds(lo + side * (size // 2), size // 2)
        return remote(st1.at[s, rows], r1.at[s, rows], r1_send.at[w, side, s], r1_recv.at[w, side, s], (right, left)[side])

    def rs_near(part, r, side):
        _, w, lo, size = part
        s = lax.rem(r, 4)
        rows = pl.ds(lo, size)
        return remote(st2.at[lax.rem(r, 2), side, rows], r2.at[s, side, rows], r2_send.at[w, side, s], r2_recv.at[w, side, s], (right, left)[side])

    def out_copy(part, r):
        _, w, lo, size = part
        s = lax.rem(r, 2)
        to = gg_ref.at[jnp.where(r < tiles, r, r - 4)] if w == 0 else gd_ref.at[r - 4]
        return pltpu.make_async_copy(gout.at[s, pl.ds(lo, size)], to, sem_out.at[w, s])

    def rs_serve(t):
        for part in parts:
            has, w, lo, size = part
            r = t - 4
            @when(has(r))
            def _():
                s, s2 = lax.rem(r, 4), lax.rem(r, 2)
                rs_near(part, r, 0).wait()
                rs_near(part, r, 1).wait()
                @when(r >= 4 * w + 2)
                def _():
                    out_copy(part, r).wait()
                def body(rows):
                    g = total(r, i, rows) + r2[s, 0, rows].astype(F32) + r2[s, 1, rows].astype(F32)
                    g = g.astype(BF16)
                    gout[s2, rows] = g
                    g = g.astype(F32)
                    sq[...] += jnp.sum((g * g).reshape(LANES // 8, 8, LANES), axis=0)
                blocks(lo, 0, size // LANES, body)
                out_copy(part, r).start()
        for part in parts:
            has, _, lo, size = part
            r = t - 2
            @when(has(r))
            def _():
                s2 = lax.rem(r, 2)
                rs_far(part, r, 0).wait()
                rs_far(part, r, 1).wait()
                half = size // 2 // LANES
                for side, j in ((0, ir), (1, il)):
                    def with_more(rows):
                        st2[s2, side, rows] = (total(r, j, rows) + r1[s2, rows].astype(F32)).astype(BF16)
                    def without(rows):
                        st2[s2, side, rows] = total(r, j, rows).astype(BF16)
                    blocks(lo, side * half, half, with_more)
                    blocks(lo, half - side * half, half, without)
                    rs_near(part, r, side).start()
        for part in parts:
            has, _, lo, size = part
            r = t - 1
            @when(has(r))
            def _():
                s2 = lax.rem(r, 2)
                rs_cores(part, r).wait()
                def body(rows):
                    st1[s2, rows] = total(r, io, rows).astype(BF16)
                blocks(lo, 0, size // LANES, body)
                rs_far(part, r, 0).start()
                rs_far(part, r, 1).start()

    def rs_begin(r):
        @when(has_rs_gu(r))
        def _():
            rs_cores(parts[0], r).start()
        @when(has_rs_d(r))
        def _():
            @when(r < tiles + 4)
            def _():
                s, k = lax.rem(r, 4), lax.rem(r, 4)
                cs = lax.rem(r // 4 - 1, 2)
                def body(dev):
                    cc, j = dev // chips, lax.rem(dev, chips)
                    own[s, cc, j, pl.ds(full_gu, full_d)] = dto[cs, cc, j, pl.ds(pl.multiple_of(k * full_d, full_d), full_d)]
                loop(0, n, body)
            rs_cores(parts[1], r).start()

    def back(g, u, dp):
        sig = 0.5 * jnp.tanh(0.5 * g) + 0.5
        silu = g * sig
        dp = dp.astype(BF16).astype(F32)
        return silu, (dp * u * (sig * (1 + g * (1 - sig)))).astype(BF16), (dp * silu).astype(BF16)

    def gate_up(s):
        return jnp.concatenate([gsl[s, :, b].reshape(d, LANES) for b in range(4)], axis=1)

    def down_tile(s, q):
        return wdr[s, pl.ds(2 * q, 2)].reshape(TILE, d)

    def gate_up_grads(r):
        s, m = lax.rem(r, 4), d // 2
        def body(k):
            val = dot(at[pl.ds(pl.multiple_of(k * m, m), m)], pbuf[:, TILE : 3 * TILE]).astype(BF16)
            for e in range(m // TILE):
                for cc in range(2):
                    lo = TILE * e + LANES * cc
                    for b in range(4):
                        own[s, cc, 2 * k + e, LANES * b : LANES * b + LANES] = val[lo : lo + LANES, LANES * b : LANES * b + LANES]
        loop(0, 2, body)

    def down_grads_one(t):
        cs, q, m = lax.rem(t // 4, 2), lax.rem(t, 4), d // 2
        def body(k):
            rows = pl.ds(pl.multiple_of(k * m, m), m)
            val = dot(dyt[rows], pbuf[:, :TILE]).astype(BF16)
            for cc in range(2):
                dto[cs, cc, q, rows] = val[:, LANES * cc : LANES * cc + LANES]
        loop(0, 2, body)

    def down_grads_zero(t, r):
        s = lax.rem(r, 4)
        val = dot(dyt[pl.ds(pl.multiple_of(lax.rem(t, 4) * TILE, TILE), TILE)], a[...]).astype(BF16)
        for dev in range(n):
            own[s, dev % 2, dev // 2, full_gu:] = val[:, LANES * dev : LANES * dev + LANES]

    def norm_rows(h):
        wide = h.astype(F32)
        scale = lax.rsqrt(jnp.mean(wide * wide, -1, keepdims=True) + 1e-6)
        return (wide * scale).astype(BF16)

    barrier = pltpu.get_barrier_semaphore()
    for k in range(1, n):
        pl.semaphore_signal(barrier, inc=1, device_id={"dp": lax.rem(me + k, n)}, device_id_type=MESH)
    for k in range(3):
        own_d(k).start()
    sq[...] = jnp.zeros_like(sq)
    pl.semaphore_wait(barrier, n - 1)

    def prologue(k):
        ag_step(k - 4)
        in_copy(k, 0).wait()
        in_copy(k, 1).wait()
        rows = pl.ds(pl.multiple_of(k * rb, rb), rb)
        av = norm_rows(a[rows])
        a[rows] = av
        at[:, rows] = av.T
        dyt[:, rows] = dyb[rows].T
        acc[rows] = jnp.zeros_like(acc[rows])
    loop(0, 4, prologue)
    a0t_copy = pltpu.make_async_copy(at, a0t_ref, sem_h.at[0])
    a0t_copy.start()

    def stg_copy(t, m):
        return pltpu.make_async_copy(stg, gu0_ref.at[t, :, pl.ds(pl.multiple_of(m * mf, mf), mf)], sem_stg)

    def p_copy(t):
        q = lax.rem(t, 4)
        cols = pl.ds(pl.multiple_of(q * TILE, TILE), TILE)
        return pltpu.make_async_copy(pbuf.at[:, cols], p0_ref.at[t // 4, :, cols], sem_p.at[q])

    def forward(t):
        ag_step(t)
        q, ch = lax.rem(t, 4), t // 4
        s = lax.rem(t, SLOTS)
        @when((q == 1) & (t > 4))
        def _():
            stash((t - 5) // 4).wait()
        @when(t >= 4)
        def _():
            p_copy(t).wait()
        def rows_of(m):
            rows = pl.ds(pl.multiple_of(m * mf, mf), mf)
            val = dot(a[rows], gate_up(s))
            g, u = val[:, :TILE], val[:, TILE:]
            @when((m > 0) | (t > 0))
            def _():
                stg_copy(t, m).wait()
            stg[0] = g
            stg[1] = u
            stg_copy(t, m).start()
            sig = 0.5 * jnp.tanh(0.5 * g) + 0.5
            pbuf[rows, pl.ds(pl.multiple_of(q * TILE, TILE), TILE)] = (g * sig * u).astype(BF16)
        loop(0, tokens // mf, rows_of)
        p_copy(t).start()
        @when(q == 3)
        def _():
            stash(ch).start()
            def down(m):
                rows = pl.ds(pl.multiple_of(m * mf, mf), mf)
                acc[rows] += dot(pbuf[rows], wdr[ch].reshape(d, d))
            loop(0, tokens // mf, down)
    loop(0, tiles, forward)
    stg_copy(0, 0).wait()
    for q in range(4):
        p_copy(q).wait()
    a0t_copy.wait()

    def x_again(k):
        rows = pl.ds(pl.multiple_of(k * rb, rb), rb)
        return pltpu.make_async_copy(x_ref.at[0, rows], pbuf.at[rows], sem_in.at[0, k])

    def h_out(k):
        rows = pl.ds(pl.multiple_of(k * rb, rb), rb)
        return pltpu.make_async_copy(pbuf.at[rows], h1_ref.at[rows], sem_in.at[1, k])

    for k in range(4):
        x_again(k).start()

    def between(k):
        ag_step(tiles + k)
        @when(k == 1)
        def _():
            stash(2).wait()
        x_again(k).wait()
        rows = pl.ds(pl.multiple_of(k * rb, rb), rb)
        h = (pbuf[rows].astype(F32) + acc[rows].astype(BF16).astype(F32)).astype(BF16)
        pbuf[rows] = h
        h_out(k).start()
        av = norm_rows(h)
        a[rows] = av
        at[:, rows] = av.T
        acc[rows] = jnp.zeros_like(acc[rows])
    loop(0, 4, between)
    for k in range(4):
        h_out(k).wait()

    def layer_one(t):
        ag_step(tiles + 4 + t)
        q, ch = lax.rem(t, 4), t // 4
        s = lax.rem(tiles + t, SLOTS)
        def rows_of(m):
            rows = pl.ds(pl.multiple_of(m * mb, mb), mb)
            val = dot(a[rows], gate_up(s))
            g, u = val[:, :TILE], val[:, TILE:]
            dp = dot_nt(dyb[rows], down_tile(ch, q))
            silu, dg, du = back(g, u, dp)
            pbuf[rows, :TILE] = (silu * u).astype(BF16)
            pbuf[rows, TILE : 2 * TILE] = dg
            pbuf[rows, 2 * TILE : 3 * TILE] = du
            acc[rows] += dot_nt(jnp.concatenate([dg, du], axis=1), gate_up(s))
        loop(0, tokens // mb, rows_of)
        rs_serve(t)
        gate_up_grads(t)
        down_grads_one(t)
        rs_begin(t)
    loop(0, tiles, layer_one)

    def h_in(k):
        rows = pl.ds(pl.multiple_of(k * rb, rb), rb)
        return pltpu.make_async_copy(h1_ref.at[rows], pbuf.at[rows], sem_in.at[1, k])

    for k in range(4):
        h_in(k).start()
    a0t_in = pltpu.make_async_copy(a0t_ref, at, sem_h.at[0])
    a0t_in.start()
    wd0_in = pltpu.make_async_copy(wd0_ref, wdr, sem_stash)
    wd0_in.start()

    def turn(k):
        rs_serve(tiles + k)
        rs_begin(tiles + k)
        h_in(k).wait()
        def part(e):
            rows = pl.ds(pl.multiple_of(k * rb + e * LANES, LANES), LANES)
            da = acc[rows].astype(BF16).astype(F32)
            wide = pbuf[rows].astype(F32)
            scale = lax.rsqrt(jnp.mean(wide * wide, -1, keepdims=True) + 1e-6)
            by_scale = jnp.sum(da * wide, -1, keepdims=True)
            by_h = (da * scale - wide * (scale * scale * scale * by_scale * (1 / d))).astype(BF16)
            dyb[rows] = (dyb[rows].astype(F32) + by_h.astype(F32)).astype(BF16)
        loop(0, rb // LANES, part)
        rows = pl.ds(pl.multiple_of(k * rb, rb), rb)
        dyt[:, rows] = dyb[rows].T
    loop(0, 4, turn)

    def gu_in(t, which):
        s = lax.rem(t, 2)
        cols = pl.ds(pl.multiple_of(2 * TILE * s + TILE * which, TILE), TILE)
        return pltpu.make_async_copy(gu0_ref.at[t, which], acc.at[:, cols], sem_h.at[1 + which + 2 * s])

    def p_in(ch):
        return pltpu.make_async_copy(p0_ref.at[ch], a, sem_p.at[0])

    gu_in(0, 0).start()
    gu_in(0, 1).start()
    a0t_in.wait()
    wd0_in.wait()

    def layer_zero(t):
        q, ch = lax.rem(t, 4), t // 4
        @when(q == 0)
        def _():
            p_in(ch).start()
        @when(t + 1 < tiles)
        def _():
            gu_in(t + 1, 0).start()
            gu_in(t + 1, 1).start()
        gu_in(t, 0).wait()
        gu_in(t, 1).wait()
        base = pl.multiple_of(2 * TILE * lax.rem(t, 2), 2 * TILE)
        def rows_of(m):
            rows = pl.ds(pl.multiple_of(m * mb, mb), mb)
            dp = dot_nt(dyb[rows], down_tile(ch, q))
            g = acc[rows, pl.ds(base, TILE)]
            u = acc[rows, pl.ds(pl.multiple_of(base + TILE, TILE), TILE)]
            _, dg, du = back(g, u, dp)
            pbuf[rows, TILE : 2 * TILE] = dg
            pbuf[rows, 2 * TILE : 3 * TILE] = du
        loop(0, tokens // mb, rows_of)
        r = tiles + 4 + t
        rs_serve(r)
        @when(q == 0)
        def _():
            p_in(ch).wait()
        gate_up_grads(r)
        down_grads_zero(t, r)
        rs_begin(r)
    loop(0, tiles, layer_zero)
    loop(steps, steps + 4, rs_serve)
    for part in parts:
        out_copy(part, steps - 2).wait()
        out_copy(part, steps - 1).wait()

    def sq_copy(k):
        return remote(sq, sqall.at[k - 1], sq_send.at[k - 1], sq_recv.at[k - 1], lax.rem(me + k, n))
    for k in range(1, n):
        sq_copy(k).start()
    for k in range(1, n):
        sq_copy(k).wait()
    ssq_ref[...] = sq[...] + jnp.sum(sqall[...], axis=0)


def run_step(x, dy, wg, wu, wd, n):
    _, tokens, d = x.shape
    layers, rows, ff = wg.shape
    tiles = ff // TILE
    any_ = pl.BlockSpec(memory_space=pl.ANY)
    dma = pltpu.SemaphoreType.DMA
    v = pltpu.VMEM
    matmul = 2 * tokens * d * ff
    return pl.pallas_call(
        functools.partial(step_kernel, n=n),
        out_shape=(
            jax.ShapeDtypeStruct((2 * tiles, 512, LANES), BF16),
            jax.ShapeDtypeStruct((2 * tiles, 256, LANES), BF16),
            jax.ShapeDtypeStruct((8, LANES), F32),
            jax.ShapeDtypeStruct((tiles, 2, tokens, TILE), F32),
            jax.ShapeDtypeStruct((3, tokens, tiles // 3 * TILE), BF16),
            jax.ShapeDtypeStruct((tokens, d), BF16),
            jax.ShapeDtypeStruct((d, tokens), BF16),
            jax.ShapeDtypeStruct((3, n, LANES, d), BF16),
        ),
        in_specs=[any_] * 5,
        out_specs=(any_, any_, pl.BlockSpec(memory_space=pltpu.VMEM), any_, any_, any_, any_, any_),
        scratch_shapes=[
            v((tokens, d), BF16), v((d, tokens), BF16), v((tokens, d), BF16), v((d, tokens), BF16),
            v((tokens, d), F32), v((tokens, d), BF16),
            v((SLOTS, n, 4, LANES, LANES), BF16), v((3, n, LANES, d), BF16),
            v((2, 2, n // 2, d, LANES), BF16), v((4, 2, n // 2, 768, LANES), BF16), v((5, n // 2, 768, LANES), BF16),
            v((2, 768, LANES), BF16), v((2, 2, 768, LANES), BF16), v((2, 768, LANES), BF16), v((4, 2, 768, LANES), BF16),
            v((2, 768, LANES), BF16), v((2, tokens // 4, TILE), F32), v((8, LANES), F32), v((n - 1, 8, LANES), F32),
            dma((2, 4)), dma(()), dma((4,)), dma((5,)), dma((2, 2)), dma((2,)), dma((3,)), dma(()),
            dma((8, SLOTS)), dma((8, SLOTS)), dma((8, SLOTS)), dma((8, SLOTS)),
            dma((2, 5)), dma((2, 5)), dma((2, 2, 2)), dma((2, 2, 2)), dma((2, 2, 4)), dma((2, 2, 4)), dma((n - 1,)), dma((n - 1,)),
        ],
        compiler_params=pltpu.CompilerParams(collective_id=0, has_side_effects=True, vmem_limit_bytes=67_000_000),
        cost_estimate=pl.CostEstimate(flops=15 * matmul, bytes_accessed=200_000_000, transcendentals=2 * tokens * ff),
        name="step",
    )(x, dy, wg, wu, wd)


def adamw_kernel(count, ssq_ref, gg_ref, gd_ref, *refs):
    ins, outs = refs[:9], refs[9:]
    mean = jnp.sum(ssq_ref[...]) / count
    factor = jnp.minimum(1.0, 0.5 * lax.rsqrt(jnp.full((8, LANES), mean, F32) + 1e-30))[0:1, 0:1]

    def update(which, rows, cols, g):
        at = (0, rows, cols)
        g = g.astype(F32) * factor
        w, m, v = (ins[3 * k + which][at] for k in range(3))
        m = 0.9 * m + 0.1 * g
        v = 0.95 * v + 0.05 * g * g
        w = w.astype(F32)
        outs[which][at] = (w - 0.02 * (m * lax.rsqrt(v + 1e-8) + 0.1 * w)).astype(BF16)
        outs[3 + which][at] = m
        outs[6 + which][at] = v

    every = slice(None)
    tiles = gg_ref.shape[0]
    for t in range(tiles):
        for b in range(4):
            col = LANES * (6 * (t % 4) + 3 * (b % 2) + t // 4)
            update(b // 2, every, slice(col, col + LANES), gg_ref[t, b])
    for ch in range(3):
        update(2, slice(LANES * ch, LANES * ch + LANES), every, gd_ref[0, ch, 0].astype(F32).T)


def run_adamw(count, ssq, gg, gd, arrays):
    layers, rows, ff = arrays[0].shape
    _, drows, d = arrays[2].shape
    tiles = ff // TILE
    parts = 4
    gg = gg.reshape(layers * tiles, 4, LANES, LANES)
    gd = gd.reshape(layers, 3, 4, 256, LANES)
    wide = pl.BlockSpec((1, rows // parts, ff), lambda l, p: (l, p, 0))
    tall = pl.BlockSpec((1, drows, d // parts), lambda l, p: (l, 0, p))
    specs = [wide, wide, tall]
    last = layers - 1
    return pl.pallas_call(
        functools.partial(adamw_kernel, count),
        grid=(layers, parts),
        out_shape=tuple(jax.ShapeDtypeStruct(a.shape, a.dtype) for a in arrays),
        in_specs=[
            pl.BlockSpec((8, LANES), lambda l, p: (0, 0)),
            pl.BlockSpec((tiles, 4, rows // parts, LANES), lambda l, p: (last - l, 0, p, 0)),
            pl.BlockSpec((1, 3, 1, 256, LANES), lambda l, p: (last - l, 0, p, 0, 0)),
        ] + specs * 3,
        out_specs=tuple(specs * 3),
        compiler_params=pltpu.CompilerParams(vmem_limit_bytes=60_000_000),
        name="adamw",
    )(ssq, gg, gd, *arrays)


def solution(mesh):
    n = mesh.shape["dp"]

    def step(x, dy, *arrays):
        gg, gd, ssq = run_step(x, dy, *arrays[:3], n)[:3]
        count = float(n * sum(w.size for w in arrays[:3]))
        return run_adamw(count, ssq, gg, gd, arrays)

    states, cut = P(("rep", "dp"), None, None), P(None, "dp", None)
    return jax.shard_map(
        step,
        mesh=mesh,
        in_specs=(states, states) + (cut,) * 9,
        out_specs=(P("rep", "dp", None),) * 9,
        check_vma=False,
    )
```

```python
import functools

import jax
import jax.numpy as jnp
from jax import lax
from jax.experimental import pallas as pl
from jax.experimental.pallas import tpu as pltpu
from jax.sharding import PartitionSpec as P

F32, BF16 = jnp.float32, jnp.bfloat16
MESH = pl.DeviceIdType.MESH
LANES = 128
TILE = 256
SLOTS = 7
NT = (((1,), (1,)), ((), ()))


def dot(a, b):
    return jnp.dot(a, b, preferred_element_type=F32)


def dot_nt(a, b):
    return lax.dot_general(a, b, NT, preferred_element_type=F32)


def loop(lo, hi, body):
    lax.fori_loop(lo, hi, lambda i, _: (body(i), None)[1], None)


def when(cond):
    return pl.when(cond)


def step_kernel(
    x_ref, dy_ref, wg_ref, wu_ref, wd_ref,
    gg_ref, gd_ref, ssq_ref, gu0_ref, p0_ref, h1_ref, a0t_ref, wd0_ref,
    a, at, dyb, dyt, acc, pbuf, gsl, wdr, dto, own, prt, st2, r1, r2, gout, stg, sq, sqall,
    sem_in, sem_stg, sem_p, sem_h, sem_out, sem_own, sem_wd, sem_stash,
    ag_send, ag_recv, dg_send, dg_recv, r0_send, r0_recv, r1_send, r1_recv, r2_send, r2_recv, sq_send, sq_recv,
    *, n,
):
    chips = n // 2
    tokens, d = a.shape
    tiles = chips * 3
    mb, mf = tokens // 2, tokens // 2
    rb = tokens // 4
    me = lax.axis_index("dp")
    i, c = me // 2, me % 2
    ir, il, io = (i + 1) % chips, (i + chips - 1) % chips, (i + 2) % chips
    right, left, opp, partner = 2 * ir + c, 2 * il + c, 2 * io + c, 2 * i + (1 - c)
    group = lax.axis_index("rep")
    h = lax.rem(group, 2)
    peer = {"rep": group + 1 - 2 * h}
    strong, weak = jnp.where(h == 0, left, right), jnp.where(h == 0, right, left)

    def remote(src, dst, send, recv, to):
        to = to if isinstance(to, dict) else {"dp": to}
        return pltpu.make_async_remote_copy(src, dst, send, recv, device_id=to, device_id_type=MESH)

    def in_copy(k, which):
        rows = pl.ds(k * rb, rb)
        return pltpu.make_async_copy((x_ref, dy_ref)[which].at[0, rows], (a, dyb)[which].at[rows], sem_in.at[which, k])

    for k in range(4):
        in_copy(k, 0).start()
        in_copy(k, 1).start()

    def has_gu(x):
        return ((x >= 0) & (x < tiles)) | ((x >= tiles + 4) & (x < 2 * tiles + 4))

    def gidx(x):
        return jnp.where(x < tiles, x, x - 4)

    def has_d(x):
        return (x >= 0) & (x < 2 * tiles)

    def gu_view(x, dev, half=None):
        s = lax.rem(gidx(x), SLOTS)
        if half is None:
            return gsl.at[s, dev]
        return gsl.at[s, dev, pl.ds(2 * half, 2)]

    def d_view(x, dev, half=None):
        s, k = lax.rem(x // 4, 3), lax.rem(x, 4)
        cols = pl.ds(pl.multiple_of(k * 256, 256), 256)
        if half is None:
            return wdr.at[s, dev, :, cols]
        return wdr.at[s, dev, pl.ds(pl.multiple_of(LANES // 2 * half, LANES // 2), LANES // 2), cols]

    streams = (
        (has_gu, gu_view, ag_send, ag_recv, lambda x: lax.rem(gidx(x), SLOTS)),
        (has_d, d_view, dg_send, dg_recv, lambda x: lax.rem(x, SLOTS)),
    )

    def own_gu(x):
        g = gidx(x)
        layer, t = g // tiles, lax.rem(g, tiles)
        ch, q = t // 4, lax.rem(t, 4)
        s = lax.rem(g, SLOTS)
        out = []
        for b in range(4):
            col = pl.multiple_of(LANES * (6 * q + 3 * (b % 2) + ch), LANES)
            src = (wg_ref, wu_ref)[b // 2].at[layer, :, pl.ds(col, LANES)]
            out.append(pltpu.make_async_copy(src, gsl.at[s, me, b], sem_own.at[lax.rem(g, 2)]))
        return out

    def own_gu_wait(x):
        g = gidx(x)
        whole = gsl.at[lax.rem(g, SLOTS), me]
        pltpu.make_async_copy(whole, whole, sem_own.at[lax.rem(g, 2)]).wait()

    def own_d(chunk):
        layer, ch = chunk // 3, lax.rem(chunk, 3)
        return pltpu.make_async_copy(wd_ref.at[layer, pl.ds(pl.multiple_of(LANES * ch, LANES), LANES)], wdr.at[ch, me], sem_wd.at[ch])

    def stash(chunk):
        return pltpu.make_async_copy(wdr.at[chunk], wd0_ref.at[chunk], sem_stash)

    def other(dev):
        return dev + 1 - 2 * lax.rem(dev, 2)

    def ag_copy(stream, x, kind):
        _, view, send, recv, sl = stream
        dev, half, to = (
            (me, None, weak), (me, h, strong), (me, None, partner),
            (weak, h, strong), (strong, h, peer), (strong, None, partner),
            (opp, h, peer), (weak, None, partner), (opp, None, partner),
        )[kind]
        v = view(x, dev, half)
        return remote(v, v, send.at[kind, sl(x)], recv.at[kind, sl(x)], to)

    def got(stream, x, kind):
        _, view, send, recv, sl = stream
        dev, half = (
            (strong, None), (weak, h), (partner, None),
            (opp, h), (weak, 1 - h), (other(strong), None),
            (opp, 1 - h), (other(weak), None), (other(opp), None),
        )[kind]
        v = view(x, dev, half)
        remote(v, v, send.at[kind, sl(x)], recv.at[kind, sl(x)], partner).wait_recv()

    def ag_stage(x, arrivals, sends):
        for stream in streams:
            @when(stream[0](x))
            def _():
                for kind in arrivals:
                    got(stream, x, kind)
                for kind in sends:
                    ag_copy(stream, x, kind).start()

    def ag_step(t):
        load, start = t + 5, t + 4
        @when(has_gu(load))
        def _():
            for cp in own_gu(load):
                cp.start()
        @when(has_d(load) & (lax.rem(load, 4) == 0) & (load >= tiles))
        def _():
            own_d(load // 4).start()
        @when(has_gu(start))
        def _():
            own_gu_wait(start)
        @when(has_d(start) & (lax.rem(start, 4) == 0))
        def _():
            own_d(start // 4).wait()
        ag_stage(start, (), (0, 1, 2))
        ag_stage(t + 3, (0, 1), (3, 4, 5))
        ag_stage(t + 2, (3, 4), (6, 7))
        ag_stage(t + 1, (6,), (8,))
        ag_stage(t, (2, 5, 7, 8), ())
        for stream in streams:
            @when(stream[0](t))
            def _():
                for kind in range(9):
                    ag_copy(stream, t, kind).wait_send()

    steps = 2 * tiles + 2
    full_d, full_gu = 2 * LANES, 4 * LANES
    packet = full_d + full_gu

    def has_rs_gu(r):
        return (r >= 0) & (r < steps)

    def has_rs_d(r):
        return ((r >= 4) & (r < tiles)) | ((r >= tiles + 2) & (r < steps))

    parts = ((has_rs_gu, 0, 0, full_gu), (has_rs_d, 1, full_gu, full_d))

    def total(r, j, rows):
        return own[lax.rem(r, 4), j, rows].astype(F32) + prt[lax.rem(r, 5), j, rows].astype(F32)

    def blocks(lo, first, count, body):
        loop(first, first + count, lambda b: body(pl.ds(pl.multiple_of(lo + b * LANES, LANES), LANES)))

    def rs_cores(part, r):
        _, w, lo, size = part
        s = lax.rem(r, 5)
        rows = pl.ds(lo, size)
        return remote(own.at[4 + lax.rem(r, 2), :, rows], prt.at[s, :, rows], r0_send.at[w, s], r0_recv.at[w, s], partner)

    def rs_far(part, r, side):
        _, w, lo, size = part
        s = lax.rem(r, 2)
        rows = pl.ds(lo + side * (size // 2), size // 2)
        src = pbuf.at[pl.ds(pl.multiple_of(s * packet + lo + side * (size // 2), LANES), size // 2), 3 * TILE : 3 * TILE + LANES]
        return remote(src, r1.at[s, rows], r1_send.at[w, side, s], r1_recv.at[w, side, s], (right, left)[side])

    def rs_near(part, r, side):
        _, w, lo, size = part
        s = lax.rem(r, 4)
        rows = pl.ds(lo, size)
        return remote(st2.at[lax.rem(r, 2), side, rows], r2.at[s, side, rows], r2_send.at[w, side, s], r2_recv.at[w, side, s], (right, left)[side])

    def out_copy(part, r):
        _, w, lo, size = part
        s = lax.rem(r, 2)
        place = jnp.where(r < tiles, r, r - 2)
        if w == 0:
            return pltpu.make_async_copy(gout.at[s, pl.ds(lo, size)], gg_ref.at[place], sem_out.at[w, s])
        place = jnp.where(r < tiles, r - 4, r - 2)
        return pltpu.make_async_copy(gout.at[s, pl.ds(lo, size)], gd_ref.at[pl.ds(pl.multiple_of(place * size, size), size)], sem_out.at[w, s])

    def out_copy_last_chunk(r):
        s = lax.rem(r, 2)
        to = gd_ref.at[pl.ds(pl.multiple_of((r - tiles + 4) * full_gu, full_gu), full_gu)]
        return pltpu.make_async_copy(gout.at[s, pl.ds(0, full_gu)], to, sem_out.at[0, s])

    def rs_serve(t):
        for part in parts:
            has, w, lo, size = part
            r = t - 4
            @when(has(r))
            def _():
                s, s2 = lax.rem(r, 4), lax.rem(r, 2)
                rs_near(part, r, 0).wait()
                rs_near(part, r, 1).wait()
                @when(r >= 4 * w + 2)
                def _():
                    out_copy(part, steps - 2 + s2).wait()
                def body(rows):
                    g = total(r, i, rows) + r2[s, 0, rows].astype(F32) + r2[s, 1, rows].astype(F32)
                    g = g.astype(BF16)
                    gout[s2, rows] = g
                    g = g.astype(F32)
                    sq[...] += jnp.sum((g * g).reshape(LANES // 8, 8, LANES), axis=0)
                blocks(lo, 0, size // LANES, body)
                if w == 0:
                    between_layers = (r >= tiles) & (r < tiles + 2)
                    @when(between_layers)
                    def _():
                        out_copy_last_chunk(r).start()
                    @when(jnp.logical_not(between_layers))
                    def _():
                        out_copy(part, r).start()
                else:
                    out_copy(part, r).start()
        for part in parts:
            has, _, lo, size = part
            r = t - 2
            @when(has(r))
            def _():
                s2 = lax.rem(r, 2)
                rs_far(part, r, 0).wait()
                rs_far(part, r, 1).wait()
                half = size // 2 // LANES
                for side, j in ((0, ir), (1, il)):
                    def with_more(rows):
                        st2[s2, side, rows] = (total(r, j, rows) + r1[s2, rows].astype(F32)).astype(BF16)
                    def without(rows):
                        st2[s2, side, rows] = total(r, j, rows).astype(BF16)
                    blocks(lo, side * half, half, with_more)
                    blocks(lo, half - side * half, half, without)
                    rs_near(part, r, side).start()
        for part in parts:
            has, _, lo, size = part
            r = t - 1
            @when(has(r))
            def _():
                s2 = lax.rem(r, 2)
                rs_cores(part, r).wait()
                def body(b):
                    rows = pl.ds(pl.multiple_of(lo + b * LANES, LANES), LANES)
                    to = pl.ds(pl.multiple_of(s2 * packet + lo + b * LANES, LANES), LANES)
                    pbuf[to, 3 * TILE : 3 * TILE + LANES] = total(r, io, rows).astype(BF16)
                loop(0, size // LANES, body)
                rs_far(part, r, 0).start()
                rs_far(part, r, 1).start()

    def rs_begin(r):
        @when(has_rs_d(r) & (r < tiles))
        def _():
            k, cs = lax.rem(r, 4), lax.rem(r // 4 - 1, 2)
            def body(dev):
                cc, j = dev // chips, lax.rem(dev, chips)
                own[place(r, cc), j, pl.ds(full_gu, full_d)] = dto[cs, cc, j, pl.ds(pl.multiple_of(k * full_d, full_d), full_d)]
            loop(0, n, body)
        for part in parts:
            @when(part[0](r))
            def _():
                rs_cores(part, r).start()

    def last_chunk(k):
        def body(dev):
            cc, j = dev // chips, lax.rem(dev, chips)
            own[place(tiles + k, cc), j, pl.ds(0, full_gu)] = dto[0, cc, j, pl.ds(pl.multiple_of(k * full_gu, full_gu), full_gu)]
        loop(0, n, body)

    def back(g, u, dp):
        sig = 0.5 * jnp.tanh(0.5 * g) + 0.5
        silu = g * sig
        dp = dp.astype(BF16).astype(F32)
        return silu, (dp * u * (sig * (1 + g * (1 - sig)))).astype(BF16), (dp * silu).astype(BF16)

    def gate_up(s):
        return jnp.concatenate([gsl[s, :, b].reshape(d, LANES) for b in range(4)], axis=1)

    def down_tile(s, q):
        return wdr[s, pl.ds(2 * q, 2)].reshape(TILE, d)

    def place(r, cc):
        return jnp.where(cc == c, lax.rem(r, 4), 4 + lax.rem(r, 2))

    def gate_up_grads(r):
        m = d // 2
        def body(k):
            val = dot(at[pl.ds(pl.multiple_of(k * m, m), m)], pbuf[:, TILE : 3 * TILE]).astype(BF16)
            for e in range(m // TILE):
                for cc in range(2):
                    lo = TILE * e + LANES * cc
                    for b in range(4):
                        own[place(r, cc), 2 * k + e, LANES * b : LANES * b + LANES] = val[lo : lo + LANES, LANES * b : LANES * b + LANES]
        loop(0, 2, body)

    def down_grads_one(t):
        cs, q, m = lax.rem(t // 4, 2), lax.rem(t, 4), d // 2
        def body(k):
            rows = pl.ds(pl.multiple_of(k * m, m), m)
            val = dot(dyt[rows], pbuf[:, :TILE]).astype(BF16)
            for cc in range(2):
                dto[cs, cc, q, rows] = val[:, LANES * cc : LANES * cc + LANES]
        loop(0, 2, body)

    def down_grads_zero(t, r):
        val = dot(dyt[pl.ds(pl.multiple_of(lax.rem(t, 4) * TILE, TILE), TILE)], a[...]).astype(BF16)
        for dev in range(n):
            own[place(r, dev % 2), dev // 2, full_gu:] = val[:, LANES * dev : LANES * dev + LANES]

    def norm_rows(h):
        wide = h.astype(F32)
        scale = lax.rsqrt(jnp.mean(wide * wide, -1, keepdims=True) + 1e-6)
        return (wide * scale).astype(BF16)

    barrier = pltpu.get_barrier_semaphore()
    for k in range(1, n):
        pl.semaphore_signal(barrier, inc=1, device_id={"dp": lax.rem(me + k, n)}, device_id_type=MESH)
    pl.semaphore_signal(barrier, inc=1, device_id=peer, device_id_type=MESH)
    for k in range(3):
        own_d(k).start()
    sq[...] = jnp.zeros_like(sq)
    pl.semaphore_wait(barrier, n)

    ag_step(-5)
    def prologue(k):
        ag_step(k - 4)
        in_copy(k, 0).wait()
        in_copy(k, 1).wait()
        rows = pl.ds(pl.multiple_of(k * rb, rb), rb)
        av = norm_rows(a[rows])
        a[rows] = av
        at[:, rows] = av.T
        dyt[:, rows] = dyb[rows].T
        acc[rows] = jnp.zeros_like(acc[rows])
    loop(0, 4, prologue)
    a0t_copy = pltpu.make_async_copy(at, a0t_ref, sem_h.at[0])
    a0t_copy.start()

    def stg_copy(t, m):
        return pltpu.make_async_copy(stg, gu0_ref.at[t, :, pl.ds(pl.multiple_of(m * mf, mf), mf)], sem_stg)

    def p_copy(t):
        q = lax.rem(t, 4)
        cols = pl.ds(pl.multiple_of(q * TILE, TILE), TILE)
        return pltpu.make_async_copy(pbuf.at[:, cols], p0_ref.at[t // 4, :, cols], sem_p.at[q])

    def forward(t):
        ag_step(t)
        q, ch = lax.rem(t, 4), t // 4
        s = lax.rem(t, SLOTS)
        @when((q == 1) & (t > 4))
        def _():
            stash((t - 5) // 4).wait()
        @when(t >= 4)
        def _():
            p_copy(t).wait()
        def rows_of(m):
            rows = pl.ds(pl.multiple_of(m * mf, mf), mf)
            val = dot(a[rows], gate_up(s))
            g, u = val[:, :TILE], val[:, TILE:]
            @when((m > 0) | (t > 0))
            def _():
                stg_copy(t, m).wait()
            stg[0] = g
            stg[1] = u
            stg_copy(t, m).start()
            sig = 0.5 * jnp.tanh(0.5 * g) + 0.5
            pbuf[rows, pl.ds(pl.multiple_of(q * TILE, TILE), TILE)] = (g * sig * u).astype(BF16)
        loop(0, tokens // mf, rows_of)
        p_copy(t).start()
        @when(q == 3)
        def _():
            stash(ch).start()
            def down(m):
                rows = pl.ds(pl.multiple_of(m * mf, mf), mf)
                acc[rows] += dot(pbuf[rows], wdr[ch].reshape(d, d))
            loop(0, tokens // mf, down)
    loop(0, tiles, forward)
    stg_copy(0, 0).wait()
    for q in range(4):
        p_copy(q).wait()
    a0t_copy.wait()

    def x_again(k):
        rows = pl.ds(pl.multiple_of(k * rb, rb), rb)
        return pltpu.make_async_copy(x_ref.at[0, rows], pbuf.at[rows], sem_in.at[0, k])

    def h_out(k):
        rows = pl.ds(pl.multiple_of(k * rb, rb), rb)
        return pltpu.make_async_copy(pbuf.at[rows], h1_ref.at[rows], sem_in.at[1, k])

    for k in range(4):
        x_again(k).start()

    def between(k):
        ag_step(tiles + k)
        @when(k == 1)
        def _():
            stash(2).wait()
        x_again(k).wait()
        rows = pl.ds(pl.multiple_of(k * rb, rb), rb)
        h = (pbuf[rows].astype(F32) + acc[rows].astype(BF16).astype(F32)).astype(BF16)
        pbuf[rows] = h
        h_out(k).start()
        av = norm_rows(h)
        a[rows] = av
        at[:, rows] = av.T
        acc[rows] = jnp.zeros_like(acc[rows])
    loop(0, 4, between)
    for k in range(4):
        h_out(k).wait()

    def layer_one(t):
        ag_step(tiles + 4 + t)
        q, ch = lax.rem(t, 4), t // 4
        s = lax.rem(tiles + t, SLOTS)
        def rows_of(m):
            rows = pl.ds(pl.multiple_of(m * mb, mb), mb)
            val = dot(a[rows], gate_up(s))
            g, u = val[:, :TILE], val[:, TILE:]
            dp = dot_nt(dyb[rows], down_tile(ch, q))
            silu, dg, du = back(g, u, dp)
            pbuf[rows, :TILE] = (silu * u).astype(BF16)
            pbuf[rows, TILE : 2 * TILE] = dg
            pbuf[rows, 2 * TILE : 3 * TILE] = du
            acc[rows] += dot_nt(jnp.concatenate([dg, du], axis=1), gate_up(s))
        loop(0, tokens // mb, rows_of)
        rs_serve(t)
        gate_up_grads(t)
        down_grads_one(t)
        rs_begin(t)
    loop(0, tiles, layer_one)

    def h_in(k):
        rows = pl.ds(pl.multiple_of(k * rb, rb), rb)
        return pltpu.make_async_copy(h1_ref.at[rows], a.at[rows], sem_in.at[1, k])

    for k in range(4):
        h_in(k).start()
    a0t_in = pltpu.make_async_copy(a0t_ref, at, sem_h.at[0])
    a0t_in.start()
    wd0_in = pltpu.make_async_copy(wd0_ref, wdr, sem_stash)
    wd0_in.start()

    def turn(k):
        @when(lax.rem(k, 2) == 0)
        def _():
            rs_serve(tiles + k // 2)
            last_chunk(k // 2)
            rs_begin(tiles + k // 2)
        h_in(k).wait()
        def part(e):
            rows = pl.ds(pl.multiple_of(k * rb + e * LANES, LANES), LANES)
            da = acc[rows].astype(BF16).astype(F32)
            wide = a[rows].astype(F32)
            scale = lax.rsqrt(jnp.mean(wide * wide, -1, keepdims=True) + 1e-6)
            by_scale = jnp.sum(da * wide, -1, keepdims=True)
            by_h = (da * scale - wide * (scale * scale * scale * by_scale * (1 / d))).astype(BF16)
            dyb[rows] = (dyb[rows].astype(F32) + by_h.astype(F32)).astype(BF16)
        loop(0, rb // LANES, part)
        rows = pl.ds(pl.multiple_of(k * rb, rb), rb)
        dyt[:, rows] = dyb[rows].T
    loop(0, 4, turn)

    def gu_in(t, which):
        s = lax.rem(t, 2)
        cols = pl.ds(pl.multiple_of(2 * TILE * s + TILE * which, TILE), TILE)
        return pltpu.make_async_copy(gu0_ref.at[t, which], acc.at[:, cols], sem_h.at[1 + which + 2 * s])

    def p_in(ch):
        return pltpu.make_async_copy(p0_ref.at[ch], a, sem_p.at[0])

    gu_in(0, 0).start()
    gu_in(0, 1).start()
    a0t_in.wait()
    wd0_in.wait()

    def layer_zero(t):
        q, ch = lax.rem(t, 4), t // 4
        @when(q == 0)
        def _():
            p_in(ch).start()
        @when(t + 1 < tiles)
        def _():
            gu_in(t + 1, 0).start()
            gu_in(t + 1, 1).start()
        gu_in(t, 0).wait()
        gu_in(t, 1).wait()
        base = pl.multiple_of(2 * TILE * lax.rem(t, 2), 2 * TILE)
        def rows_of(m):
            rows = pl.ds(pl.multiple_of(m * mb, mb), mb)
            dp = dot_nt(dyb[rows], down_tile(ch, q))
            g = acc[rows, pl.ds(base, TILE)]
            u = acc[rows, pl.ds(pl.multiple_of(base + TILE, TILE), TILE)]
            _, dg, du = back(g, u, dp)
            pbuf[rows, TILE : 2 * TILE] = dg
            pbuf[rows, 2 * TILE : 3 * TILE] = du
        loop(0, tokens // mb, rows_of)
        r = tiles + 2 + t
        rs_serve(r)
        @when(q == 0)
        def _():
            p_in(ch).wait()
        gate_up_grads(r)
        down_grads_zero(t, r)
        rs_begin(r)
    loop(0, tiles, layer_zero)
    loop(steps, steps + 4, rs_serve)
    for part in parts:
        out_copy(part, steps - 2).wait()
        out_copy(part, steps - 1).wait()

    def sq_copy(k):
        return remote(sq, sqall.at[k - 1], sq_send.at[k - 1], sq_recv.at[k - 1], lax.rem(me + k, n))
    for k in range(1, n):
        sq_copy(k).start()
    for k in range(1, n):
        sq_copy(k).wait()
    ssq_ref[...] = sq[...] + jnp.sum(sqall[...], axis=0)


def run_step(x, dy, wg, wu, wd, n):
    _, tokens, d = x.shape
    layers, rows, ff = wg.shape
    tiles = ff // TILE
    any_ = pl.BlockSpec(memory_space=pl.ANY)
    dma = pltpu.SemaphoreType.DMA
    v = pltpu.VMEM
    matmul = 2 * tokens * d * ff
    return pl.pallas_call(
        functools.partial(step_kernel, n=n),
        out_shape=(
            jax.ShapeDtypeStruct((2 * tiles, 4 * LANES, LANES), BF16),
            jax.ShapeDtypeStruct((4 * tiles * LANES, LANES), BF16),
            jax.ShapeDtypeStruct((8, LANES), F32),
            jax.ShapeDtypeStruct((tiles, 2, tokens, TILE), F32),
            jax.ShapeDtypeStruct((3, tokens, tiles // 3 * TILE), BF16),
            jax.ShapeDtypeStruct((tokens, d), BF16),
            jax.ShapeDtypeStruct((d, tokens), BF16),
            jax.ShapeDtypeStruct((3, n, LANES, d), BF16),
        ),
        in_specs=[any_] * 5,
        out_specs=(any_, any_, pl.BlockSpec(memory_space=pltpu.VMEM), any_, any_, any_, any_, any_),
        scratch_shapes=[
            v((tokens, d), BF16), v((d, tokens), BF16), v((tokens, d), BF16), v((d, tokens), BF16),
            v((tokens, d), F32), v((tokens, d), BF16),
            v((SLOTS, n, 4, LANES, LANES), BF16), v((3, n, LANES, d), BF16),
            v((2, 2, n // 2, d, LANES), BF16), v((6, n // 2, 768, LANES), BF16), v((5, n // 2, 768, LANES), BF16),
            v((2, 2, 768, LANES), BF16), v((2, 768, LANES), BF16), v((4, 2, 768, LANES), BF16),
            v((2, 768, LANES), BF16), v((2, tokens // 2, TILE), F32), v((8, LANES), F32), v((n - 1, 8, LANES), F32),
            dma((2, 4)), dma(()), dma((4,)), dma((5,)), dma((2, 2)), dma((2,)), dma((3,)), dma(()),
            dma((9, SLOTS)), dma((9, SLOTS)), dma((9, SLOTS)), dma((9, SLOTS)),
            dma((2, 5)), dma((2, 5)), dma((2, 2, 2)), dma((2, 2, 2)), dma((2, 2, 4)), dma((2, 2, 4)), dma((n - 1,)), dma((n - 1,)),
        ],
        compiler_params=pltpu.CompilerParams(collective_id=0, has_side_effects=True, vmem_limit_bytes=67_000_000),
        cost_estimate=pl.CostEstimate(flops=15 * matmul, bytes_accessed=200_000_000, transcendentals=2 * tokens * ff),
        name="step",
    )(x, dy, wg, wu, wd)


def adamw_kernel(count, ssq_ref, gg_ref, gd_ref, *refs):
    ins, outs = refs[:9], refs[9:]
    mean = jnp.sum(ssq_ref[...]) / count
    factor = jnp.minimum(1.0, 0.5 * lax.rsqrt(jnp.full((8, LANES), mean, F32) + 1e-30))[0:1, 0:1]

    def update(which, rows, cols, g):
        at = (0, rows, cols)
        g = g.astype(F32) * factor
        w, m, v = (ins[3 * k + which][at] for k in range(3))
        m = 0.9 * m + 0.1 * g
        v = 0.95 * v + 0.05 * g * g
        w = w.astype(F32)
        outs[which][at] = (w - 0.02 * (m * lax.rsqrt(v + 1e-8) + 0.1 * w)).astype(BF16)
        outs[3 + which][at] = m
        outs[6 + which][at] = v

    every = slice(None)
    tiles = gg_ref.shape[0]
    for t in range(tiles):
        for b in range(4):
            col = LANES * (6 * (t % 4) + 3 * (b % 2) + t // 4)
            update(b // 2, every, slice(col, col + LANES), gg_ref[t, b])
    for ch in range(3):
        update(2, slice(LANES * ch, LANES * ch + LANES), every, gd_ref[0, ch, 0].astype(F32).T)


def run_adamw(count, ssq, gg, gd, arrays):
    layers, rows, ff = arrays[0].shape
    _, drows, d = arrays[2].shape
    tiles = ff // TILE
    parts = 4
    gg = gg.reshape(layers * tiles, 4, LANES, LANES)
    gd = gd.reshape(layers, 3, 4, 256, LANES)
    wide = pl.BlockSpec((1, rows // parts, ff), lambda l, p: (l, p, 0))
    tall = pl.BlockSpec((1, drows, d // parts), lambda l, p: (l, 0, p))
    specs = [wide, wide, tall]
    last = layers - 1
    return pl.pallas_call(
        functools.partial(adamw_kernel, count),
        grid=(layers, parts),
        out_shape=tuple(jax.ShapeDtypeStruct(a.shape, a.dtype) for a in arrays),
        in_specs=[
            pl.BlockSpec((8, LANES), lambda l, p: (0, 0)),
            pl.BlockSpec((tiles, 4, rows // parts, LANES), lambda l, p: (last - l, 0, p, 0)),
            pl.BlockSpec((1, 3, 1, 256, LANES), lambda l, p: (last - l, 0, p, 0, 0)),
        ] + specs * 3,
        out_specs=tuple(specs * 3),
        compiler_params=pltpu.CompilerParams(vmem_limit_bytes=60_000_000),
        name="adamw",
    )(ssq, gg, gd, *arrays)


def solution(mesh):
    n = mesh.shape["dp"]

    def step(x, dy, *arrays):
        gg, gd, ssq = run_step(x, dy, *arrays[:3], n)[:3]
        count = float(n * sum(w.size for w in arrays[:3]))
        return run_adamw(count, ssq, gg, gd, arrays)

    states, cut = P(("rep", "dp"), None, None), P(None, "dp", None)
    return jax.shard_map(
        step,
        mesh=mesh,
        in_specs=(states, states) + (cut,) * 9,
        out_specs=(P("rep", "dp", None),) * 9,
        check_vma=False,
    )
```

```python
import functools

import jax
import jax.numpy as jnp
from jax import lax
from jax.experimental import pallas as pl
from jax.experimental.pallas import tpu as pltpu
from jax.sharding import PartitionSpec as P

F32, BF16 = jnp.float32, jnp.bfloat16
MESH = pl.DeviceIdType.MESH
LANES = 128
TILE = 256
SLOTS = 7
NT = (((1,), (1,)), ((), ()))


def dot(a, b):
    return jnp.dot(a, b, preferred_element_type=F32)


def dot_nt(a, b):
    return lax.dot_general(a, b, NT, preferred_element_type=F32)


def loop(lo, hi, body):
    lax.fori_loop(lo, hi, lambda i, _: (body(i), None)[1], None)


def when(cond):
    return pl.when(cond)


def step_kernel(
    x_ref, dy_ref, wg_ref, wu_ref, wd_ref,
    gg_ref, gd_ref, ssq_ref, gu0_ref, p0_ref, h1_ref, a0t_ref, wd0_ref,
    a, at, dyb, dyt, acc, pbuf, gsl, wdr, dto, own, prt, st1, st2, r1, r2, gout, stg, sq, sqall,
    sem_in, sem_stg, sem_p, sem_h, sem_out, sem_own, sem_wd, sem_stash,
    ag_send, ag_recv, dg_send, dg_recv, r0_send, r0_recv, r1_send, r1_recv, r2_send, r2_recv, sq_send, sq_recv,
    *, n,
):
    chips = n // 2
    tokens, d = a.shape
    tiles = chips * 3
    mb, mf = tokens // 2, tokens // 2
    rb = tokens // 4
    me = lax.axis_index("dp")
    i, c = me // 2, me % 2
    ir, il, io = (i + 1) % chips, (i + chips - 1) % chips, (i + 2) % chips
    right, left, opp, partner = 2 * ir + c, 2 * il + c, 2 * io + c, 2 * i + (1 - c)
    group = lax.axis_index("rep")
    h = lax.rem(group, 2)
    peer = {"rep": group + 1 - 2 * h}
    strong, weak = jnp.where(h == 0, left, right), jnp.where(h == 0, right, left)

    def remote(src, dst, send, recv, to):
        to = to if isinstance(to, dict) else {"dp": to}
        return pltpu.make_async_remote_copy(src, dst, send, recv, device_id=to, device_id_type=MESH)

    def in_copy(k, which):
        rows = pl.ds(k * rb, rb)
        return pltpu.make_async_copy((x_ref, dy_ref)[which].at[0, rows], (a, dyb)[which].at[rows], sem_in.at[which, k])

    for k in range(4):
        in_copy(k, 0).start()
        in_copy(k, 1).start()

    def has_gu(x):
        return ((x >= 0) & (x < tiles)) | ((x >= tiles + 4) & (x < 2 * tiles + 4))

    def gidx(x):
        return jnp.where(x < tiles, x, x - 4)

    def has_d(x):
        return (x >= 0) & (x < 2 * tiles)

    def gu_view(x, dev, half=None):
        s = lax.rem(gidx(x), SLOTS)
        if half is None:
            return gsl.at[s, dev]
        return gsl.at[s, dev, pl.ds(2 * half, 2)]

    def d_view(x, dev, half=None):
        s, k = lax.rem(x // 4, 3), lax.rem(x, 4)
        cols = pl.ds(pl.multiple_of(k * 256, 256), 256)
        if half is None:
            return wdr.at[s, dev, :, cols]
        return wdr.at[s, dev, pl.ds(pl.multiple_of(LANES // 2 * half, LANES // 2), LANES // 2), cols]

    streams = (
        (has_gu, gu_view, ag_send, ag_recv, lambda x: lax.rem(gidx(x), SLOTS)),
        (has_d, d_view, dg_send, dg_recv, lambda x: lax.rem(x, SLOTS)),
    )

    def own_gu(x):
        g = gidx(x)
        layer, t = g // tiles, lax.rem(g, tiles)
        ch, q = t // 4, lax.rem(t, 4)
        s = lax.rem(g, SLOTS)
        out = []
        for b in range(4):
            col = pl.multiple_of(LANES * (6 * q + 3 * (b % 2) + ch), LANES)
            src = (wg_ref, wu_ref)[b // 2].at[layer, :, pl.ds(col, LANES)]
            out.append(pltpu.make_async_copy(src, gsl.at[s, me, b], sem_own.at[lax.rem(g, 2)]))
        return out

    def own_gu_wait(x):
        g = gidx(x)
        whole = gsl.at[lax.rem(g, SLOTS), me]
        pltpu.make_async_copy(whole, whole, sem_own.at[lax.rem(g, 2)]).wait()

    def own_d(chunk):
        layer, ch = chunk // 3, lax.rem(chunk, 3)
        return pltpu.make_async_copy(wd_ref.at[layer, pl.ds(pl.multiple_of(LANES * ch, LANES), LANES)], wdr.at[ch, me], sem_wd.at[ch])

    def stash(chunk):
        return pltpu.make_async_copy(wdr.at[chunk], wd0_ref.at[chunk], sem_stash)

    def other(dev):
        return dev + 1 - 2 * lax.rem(dev, 2)

    def ag_copy(stream, x, kind):
        _, view, send, recv, sl = stream
        dev, half, to = (
            (me, None, weak), (me, h, strong), (me, None, partner),
            (weak, h, strong), (strong, h, peer), (strong, None, partner),
            (opp, h, peer), (weak, None, partner), (opp, None, partner),
        )[kind]
        v = view(x, dev, half)
        return remote(v, v, send.at[kind, sl(x)], recv.at[kind, sl(x)], to)

    def got(stream, x, kind):
        _, view, send, recv, sl = stream
        dev, half = (
            (strong, None), (weak, h), (partner, None),
            (opp, h), (weak, 1 - h), (other(strong), None),
            (opp, 1 - h), (other(weak), None), (other(opp), None),
        )[kind]
        v = view(x, dev, half)
        remote(v, v, send.at[kind, sl(x)], recv.at[kind, sl(x)], partner).wait_recv()

    def ag_stage(x, arrivals, sends):
        for stream in streams:
            @when(stream[0](x))
            def _():
                for kind in arrivals:
                    got(stream, x, kind)
                for kind in sends:
                    ag_copy(stream, x, kind).start()

    def ag_step(t):
        load, start = t + 5, t + 4
        @when(has_gu(load))
        def _():
            for cp in own_gu(load):
                cp.start()
        @when(has_d(load) & (lax.rem(load, 4) == 0) & (load >= tiles))
        def _():
            own_d(load // 4).start()
        @when(has_gu(start))
        def _():
            own_gu_wait(start)
        @when(has_d(start) & (lax.rem(start, 4) == 0))
        def _():
            own_d(start // 4).wait()
        ag_stage(start, (), (0, 1, 2))
        ag_stage(t + 3, (0, 1), (3, 4, 5))
        ag_stage(t + 2, (3, 4), (6, 7))
        ag_stage(t + 1, (6,), (8,))
        ag_stage(t, (2, 5, 7, 8), ())
        for stream in streams:
            @when(stream[0](t))
            def _():
                for kind in range(9):
                    ag_copy(stream, t, kind).wait_send()

    steps = 2 * tiles + 2
    full_d, full_gu = 2 * LANES, 4 * LANES

    def has_rs_gu(r):
        return (r >= 0) & (r < steps)

    def has_rs_d(r):
        return ((r >= 4) & (r < tiles)) | ((r >= tiles + 2) & (r < steps))

    parts = ((has_rs_gu, 0, 0, full_gu), (has_rs_d, 1, full_gu, full_d))

    def total(r, j, rows):
        return own[lax.rem(r, 4), j, rows].astype(F32) + prt[lax.rem(r, 5), j, rows].astype(F32)

    def blocks(lo, first, count, body):
        loop(first, first + count, lambda b: body(pl.ds(pl.multiple_of(lo + b * LANES, LANES), LANES)))

    def rs_cores(part, r):
        _, w, lo, size = part
        s = lax.rem(r, 5)
        rows = pl.ds(lo, size)
        return remote(own.at[4 + lax.rem(r, 2), :, rows], prt.at[s, :, rows], r0_send.at[w, s], r0_recv.at[w, s], partner)

    def rs_far(part, r, side):
        _, w, lo, size = part
        s = lax.rem(r, 2)
        rows = pl.ds(lo + side * (size // 2), size // 2)
        return remote(st1.at[s, rows], r1.at[s, rows], r1_send.at[w, side, s], r1_recv.at[w, side, s], (right, left)[side])

    def rs_near(part, r, side):
        _, w, lo, size = part
        s = lax.rem(r, 4)
        rows = pl.ds(lo, size)
        return remote(st2.at[lax.rem(r, 2), side, rows], r2.at[s, side, rows], r2_send.at[w, side, s], r2_recv.at[w, side, s], (right, left)[side])

    def out_copy(part, r):
        _, w, lo, size = part
        s = lax.rem(r, 2)
        place = jnp.where(r < tiles, r, r - 2)
        if w == 0:
            return pltpu.make_async_copy(gout.at[s, pl.ds(lo, size)], gg_ref.at[place], sem_out.at[w, s])
        place = jnp.where(r < tiles, r - 4, r - 2)
        return pltpu.make_async_copy(gout.at[s, pl.ds(lo, size)], gd_ref.at[pl.ds(pl.multiple_of(place * size, size), size)], sem_out.at[w, s])

    def out_copy_last_chunk(r):
        s = lax.rem(r, 2)
        to = gd_ref.at[pl.ds(pl.multiple_of((r - tiles + 4) * full_gu, full_gu), full_gu)]
        return pltpu.make_async_copy(gout.at[s, pl.ds(0, full_gu)], to, sem_out.at[0, s])

    def rs_serve(t):
        for part in parts:
            has, w, lo, size = part
            r = t - 4
            @when(has(r))
            def _():
                s, s2 = lax.rem(r, 4), lax.rem(r, 2)
                rs_near(part, r, 0).wait()
                rs_near(part, r, 1).wait()
                @when(r >= 4 * w + 2)
                def _():
                    out_copy(part, steps - 2 + s2).wait()
                def body(rows):
                    g = total(r, i, rows) + r2[s, 0, rows].astype(F32) + r2[s, 1, rows].astype(F32)
                    g = g.astype(BF16)
                    gout[s2, rows] = g
                    g = g.astype(F32)
                    sq[...] += jnp.sum((g * g).reshape(LANES // 8, 8, LANES), axis=0)
                blocks(lo, 0, size // LANES, body)
                if w == 0:
                    between_layers = (r >= tiles) & (r < tiles + 2)
                    @when(between_layers)
                    def _():
                        out_copy_last_chunk(r).start()
                    @when(jnp.logical_not(between_layers))
                    def _():
                        out_copy(part, r).start()
                else:
                    out_copy(part, r).start()
        for part in parts:
            has, _, lo, size = part
            r = t - 2
            @when(has(r))
            def _():
                s2 = lax.rem(r, 2)
                rs_far(part, r, 0).wait()
                rs_far(part, r, 1).wait()
                half = size // 2 // LANES
                for side, j in ((0, ir), (1, il)):
                    def with_more(rows):
                        st2[s2, side, rows] = (total(r, j, rows) + r1[s2, rows].astype(F32)).astype(BF16)
                    def without(rows):
                        st2[s2, side, rows] = total(r, j, rows).astype(BF16)
                    blocks(lo, side * half, half, with_more)
                    blocks(lo, half - side * half, half, without)
                    rs_near(part, r, side).start()
        for part in parts:
            has, _, lo, size = part
            r = t - 1
            @when(has(r))
            def _():
                s2 = lax.rem(r, 2)
                rs_cores(part, r).wait()
                def body(rows):
                    st1[s2, rows] = total(r, io, rows).astype(BF16)
                blocks(lo, 0, size // LANES, body)
                rs_far(part, r, 0).start()
                rs_far(part, r, 1).start()

    def rs_begin(r):
        @when(has_rs_d(r) & (r < tiles))
        def _():
            k, cs = lax.rem(r, 4), lax.rem(r // 4 - 1, 2)
            def body(dev):
                cc, j = dev // chips, lax.rem(dev, chips)
                own[place(r, cc), j, pl.ds(full_gu, full_d)] = dto[cs, cc, j, pl.ds(pl.multiple_of(k * full_d, full_d), full_d)]
            loop(0, n, body)
        for part in parts:
            @when(part[0](r))
            def _():
                rs_cores(part, r).start()

    def last_chunk(k):
        def body(dev):
            cc, j = dev // chips, lax.rem(dev, chips)
            own[place(tiles + k, cc), j, pl.ds(0, full_gu)] = dto[0, cc, j, pl.ds(pl.multiple_of(k * full_gu, full_gu), full_gu)]
        loop(0, n, body)

    def back(g, u, dp):
        sig = 0.5 * jnp.tanh(0.5 * g) + 0.5
        silu = g * sig
        dp = dp.astype(F32)
        return silu, (dp * u * (sig * (1 + g * (1 - sig)))).astype(BF16), (dp * silu).astype(BF16)

    def gate_up(s):
        return jnp.concatenate([gsl[s, :, b].reshape(d, LANES) for b in range(4)], axis=1)

    def dp_pair(ch, q):
        def rows_of(m):
            rows = pl.ds(pl.multiple_of(m * mb, mb), mb)
            val = dot_nt(dyb[rows], wdr[ch, pl.ds(2 * q, 4)].reshape(2 * TILE, d)).astype(BF16)
            pbuf[rows, :TILE] = val[:, :TILE]
            pbuf[rows, 3 * TILE :] = val[:, TILE:]
        loop(0, tokens // mb, rows_of)

    def place(r, cc):
        return jnp.where(cc == c, lax.rem(r, 4), 4 + lax.rem(r, 2))

    def weight_grads(r, t=None):
        m = d // 2
        def body(k):
            rows = pl.ds(pl.multiple_of(k * m, m), m)
            val = dot(at[rows], pbuf[:, TILE : 3 * TILE]).astype(BF16)
            if t is not None:
                cs, q = lax.rem(t // 4, 2), lax.rem(t, 4)
                more = dot(dyt[rows], pbuf[:, :TILE]).astype(BF16)
                for cc in range(2):
                    dto[cs, cc, q, rows] = more[:, LANES * cc : LANES * cc + LANES]
            for e in range(m // TILE):
                for cc in range(2):
                    lo = TILE * e + LANES * cc
                    for b in range(4):
                        own[place(r, cc), 2 * k + e, LANES * b : LANES * b + LANES] = val[lo : lo + LANES, LANES * b : LANES * b + LANES]
        loop(0, 2, body)

    def down_grads_zero(t, r):
        val = dot(dyt[pl.ds(pl.multiple_of(lax.rem(t, 4) * TILE, TILE), TILE)], a[...]).astype(BF16)
        for dev in range(n):
            own[place(r, dev % 2), dev // 2, full_gu:] = val[:, LANES * dev : LANES * dev + LANES]

    def norm_rows(h):
        wide = h.astype(F32)
        scale = lax.rsqrt(jnp.mean(wide * wide, -1, keepdims=True) + 1e-6)
        return (wide * scale).astype(BF16)

    barrier = pltpu.get_barrier_semaphore()
    for k in range(1, n):
        pl.semaphore_signal(barrier, inc=1, device_id={"dp": lax.rem(me + k, n)}, device_id_type=MESH)
    pl.semaphore_signal(barrier, inc=1, device_id=peer, device_id_type=MESH)
    for k in range(3):
        own_d(k).start()
    sq[...] = jnp.zeros_like(sq)
    pl.semaphore_wait(barrier, n)

    ag_step(-5)
    def prologue(k):
        ag_step(k - 4)
        in_copy(k, 0).wait()
        in_copy(k, 1).wait()
        rows = pl.ds(pl.multiple_of(k * rb, rb), rb)
        av = norm_rows(a[rows])
        a[rows] = av
        at[:, rows] = av.T
        dyt[:, rows] = dyb[rows].T
        acc[rows] = jnp.zeros_like(acc[rows])
    loop(0, 4, prologue)
    a0t_copy = pltpu.make_async_copy(at, a0t_ref, sem_h.at[0])
    a0t_copy.start()

    def stg_copy(slot, t, row):
        return pltpu.make_async_copy(stg.at[slot], gu0_ref.at[t, :, pl.ds(pl.multiple_of(row, TILE), TILE)], sem_stg.at[slot])

    def p_copy(t):
        q = lax.rem(t, 4)
        cols = pl.ds(pl.multiple_of(q * TILE, TILE), TILE)
        return pltpu.make_async_copy(pbuf.at[:, cols], p0_ref.at[t // 4, :, cols], sem_p.at[q])

    def forward(t):
        ag_step(t)
        q, ch = lax.rem(t, 4), t // 4
        s = lax.rem(t, SLOTS)
        @when((q == 1) & (t > 4))
        def _():
            stash((t - 5) // 4).wait()
        @when(t >= 4)
        def _():
            p_copy(t).wait()
        def rows_of(m):
            rows = pl.ds(pl.multiple_of(m * mf, mf), mf)
            val = dot(a[rows], gate_up(s))
            g, u = val[:, :TILE], val[:, TILE:]
            for e in range(mf // TILE):
                turn_no = t * (tokens // TILE) + m * (mf // TILE) + e
                slot = lax.rem(turn_no, 3)
                @when(turn_no >= 3)
                def _():
                    stg_copy(slot, 0, 0).wait()
                stg[slot, 0] = g[TILE * e : TILE * e + TILE]
                stg[slot, 1] = u[TILE * e : TILE * e + TILE]
                stg_copy(slot, t, m * mf + TILE * e).start()
            sig = 0.5 * jnp.tanh(0.5 * g) + 0.5
            pbuf[rows, pl.ds(pl.multiple_of(q * TILE, TILE), TILE)] = (g * sig * u).astype(BF16)
        loop(0, tokens // mf, rows_of)
        p_copy(t).start()
        @when(q == 3)
        def _():
            stash(ch).start()
            def down(m):
                rows = pl.ds(pl.multiple_of(m * mf, mf), mf)
                acc[rows] += dot(pbuf[rows], wdr[ch].reshape(d, d))
            loop(0, tokens // mf, down)
    loop(0, tiles, forward)
    for slot in range(3):
        stg_copy(slot, 0, 0).wait()
    for q in range(4):
        p_copy(q).wait()
    a0t_copy.wait()

    def x_again(k):
        rows = pl.ds(pl.multiple_of(k * rb, rb), rb)
        return pltpu.make_async_copy(x_ref.at[0, rows], pbuf.at[rows], sem_in.at[0, k])

    def h_out(k):
        rows = pl.ds(pl.multiple_of(k * rb, rb), rb)
        return pltpu.make_async_copy(pbuf.at[rows], h1_ref.at[rows], sem_in.at[1, k])

    for k in range(4):
        x_again(k).start()

    def between(k):
        ag_step(tiles + k)
        @when(k == 1)
        def _():
            stash(2).wait()
        x_again(k).wait()
        rows = pl.ds(pl.multiple_of(k * rb, rb), rb)
        h = (pbuf[rows].astype(F32) + acc[rows].astype(BF16).astype(F32)).astype(BF16)
        pbuf[rows] = h
        h_out(k).start()
        av = norm_rows(h)
        a[rows] = av
        at[:, rows] = av.T
        acc[rows] = jnp.zeros_like(acc[rows])
    loop(0, 4, between)
    for k in range(4):
        h_out(k).wait()

    def layer_one(t):
        ag_step(tiles + 4 + t)
        q, ch = lax.rem(t, 4), t // 4
        s = lax.rem(tiles + t, SLOTS)
        @when(lax.rem(q, 2) == 0)
        def _():
            dp_pair(ch, q)
        dp_at = pl.multiple_of(3 * TILE * lax.rem(q, 2), TILE)
        def rows_of(m):
            rows = pl.ds(pl.multiple_of(m * mb, mb), mb)
            val = dot(a[rows], gate_up(s))
            g, u = val[:, :TILE], val[:, TILE:]
            silu, dg, du = back(g, u, pbuf[rows, pl.ds(dp_at, TILE)])
            pbuf[rows, :TILE] = (silu * u).astype(BF16)
            pbuf[rows, TILE : 2 * TILE] = dg
            pbuf[rows, 2 * TILE : 3 * TILE] = du
            acc[rows] += dot_nt(jnp.concatenate([dg, du], axis=1), gate_up(s))
        loop(0, tokens // mb, rows_of)
        rs_serve(t)
        weight_grads(t, t)
        rs_begin(t)
    loop(0, tiles, layer_one)

    def h_in(k):
        rows = pl.ds(pl.multiple_of(k * rb, rb), rb)
        return pltpu.make_async_copy(h1_ref.at[rows], a.at[rows], sem_in.at[1, k])

    for k in range(4):
        h_in(k).start()
    a0t_in = pltpu.make_async_copy(a0t_ref, at, sem_h.at[0])
    a0t_in.start()
    wd0_in = pltpu.make_async_copy(wd0_ref, wdr, sem_stash)
    wd0_in.start()

    def turn(k):
        @when(lax.rem(k, 2) == 0)
        def _():
            rs_serve(tiles + k // 2)
            last_chunk(k // 2)
            rs_begin(tiles + k // 2)
        h_in(k).wait()
        def part(e):
            rows = pl.ds(pl.multiple_of(k * rb + e * LANES, LANES), LANES)
            da = acc[rows].astype(BF16).astype(F32)
            wide = a[rows].astype(F32)
            scale = lax.rsqrt(jnp.mean(wide * wide, -1, keepdims=True) + 1e-6)
            by_scale = jnp.sum(da * wide, -1, keepdims=True)
            by_h = (da * scale - wide * (scale * scale * scale * by_scale * (1 / d))).astype(BF16)
            dyb[rows] = (dyb[rows].astype(F32) + by_h.astype(F32)).astype(BF16)
        loop(0, rb // LANES, part)
        rows = pl.ds(pl.multiple_of(k * rb, rb), rb)
        dyt[:, rows] = dyb[rows].T
    loop(0, 4, turn)

    def gu_in(t, which):
        s = lax.rem(t, 2)
        cols = pl.ds(pl.multiple_of(2 * TILE * s + TILE * which, TILE), TILE)
        return pltpu.make_async_copy(gu0_ref.at[t, which], acc.at[:, cols], sem_h.at[1 + which + 2 * s])

    def p_in(ch):
        return pltpu.make_async_copy(p0_ref.at[ch], a, sem_p.at[0])

    gu_in(0, 0).start()
    gu_in(0, 1).start()
    a0t_in.wait()
    wd0_in.wait()

    def layer_zero(t):
        q, ch = lax.rem(t, 4), t // 4
        @when(q == 0)
        def _():
            p_in(ch).start()
        @when(t + 1 < tiles)
        def _():
            gu_in(t + 1, 0).start()
            gu_in(t + 1, 1).start()
        gu_in(t, 0).wait()
        gu_in(t, 1).wait()
        base = pl.multiple_of(2 * TILE * lax.rem(t, 2), 2 * TILE)
        def rows_of(m):
            rows = pl.ds(pl.multiple_of(m * mb, mb), mb)
            dp = dot_nt(dyb[rows], wdr[ch, pl.ds(2 * q, 2)].reshape(TILE, d)).astype(BF16)
            g = acc[rows, pl.ds(base, TILE)]
            u = acc[rows, pl.ds(pl.multiple_of(base + TILE, TILE), TILE)]
            _, dg, du = back(g, u, dp)
            pbuf[rows, TILE : 2 * TILE] = dg
            pbuf[rows, 2 * TILE : 3 * TILE] = du
        loop(0, tokens // mb, rows_of)
        r = tiles + 2 + t
        rs_serve(r)
        @when(q == 0)
        def _():
            p_in(ch).wait()
        weight_grads(r)
        down_grads_zero(t, r)
        rs_begin(r)
    loop(0, tiles, layer_zero)
    loop(steps, steps + 4, rs_serve)
    for part in parts:
        out_copy(part, steps - 2).wait()
        out_copy(part, steps - 1).wait()

    def sq_copy(k):
        return remote(sq, sqall.at[k - 1], sq_send.at[k - 1], sq_recv.at[k - 1], lax.rem(me + k, n))
    for k in range(1, n):
        sq_copy(k).start()
    for k in range(1, n):
        sq_copy(k).wait()
    ssq_ref[...] = sq[...] + jnp.sum(sqall[...], axis=0)


def run_step(x, dy, wg, wu, wd, n):
    _, tokens, d = x.shape
    layers, rows, ff = wg.shape
    tiles = ff // TILE
    any_ = pl.BlockSpec(memory_space=pl.ANY)
    dma = pltpu.SemaphoreType.DMA
    v = pltpu.VMEM
    matmul = 2 * tokens * d * ff
    return pl.pallas_call(
        functools.partial(step_kernel, n=n),
        out_shape=(
            jax.ShapeDtypeStruct((2 * tiles, 4 * LANES, LANES), BF16),
            jax.ShapeDtypeStruct((4 * tiles * LANES, LANES), BF16),
            jax.ShapeDtypeStruct((8, LANES), F32),
            jax.ShapeDtypeStruct((tiles, 2, tokens, TILE), F32),
            jax.ShapeDtypeStruct((3, tokens, tiles // 3 * TILE), BF16),
            jax.ShapeDtypeStruct((tokens, d), BF16),
            jax.ShapeDtypeStruct((d, tokens), BF16),
            jax.ShapeDtypeStruct((3, n, LANES, d), BF16),
        ),
        in_specs=[any_] * 5,
        out_specs=(any_, any_, pl.BlockSpec(memory_space=pltpu.VMEM), any_, any_, any_, any_, any_),
        scratch_shapes=[
            v((tokens, d), BF16), v((d, tokens), BF16), v((tokens, d), BF16), v((d, tokens), BF16),
            v((tokens, d), F32), v((tokens, d), BF16),
            v((SLOTS, n, 4, LANES, LANES), BF16), v((3, n, LANES, d), BF16),
            v((2, 2, n // 2, d, LANES), BF16), v((6, n // 2, 768, LANES), BF16), v((5, n // 2, 768, LANES), BF16),
            v((2, 768, LANES), BF16), v((2, 2, 768, LANES), BF16), v((2, 768, LANES), BF16), v((4, 2, 768, LANES), BF16),
            v((2, 768, LANES), BF16), v((3, 2, TILE, TILE), F32), v((8, LANES), F32), v((n - 1, 8, LANES), F32),
            dma((2, 4)), dma((3,)), dma((4,)), dma((5,)), dma((2, 2)), dma((2,)), dma((3,)), dma(()),
            dma((9, SLOTS)), dma((9, SLOTS)), dma((9, SLOTS)), dma((9, SLOTS)),
            dma((2, 5)), dma((2, 5)), dma((2, 2, 2)), dma((2, 2, 2)), dma((2, 2, 4)), dma((2, 2, 4)), dma((n - 1,)), dma((n - 1,)),
        ],
        compiler_params=pltpu.CompilerParams(collective_id=0, has_side_effects=True, vmem_limit_bytes=67_000_000),
        cost_estimate=pl.CostEstimate(flops=15 * matmul, bytes_accessed=200_000_000, transcendentals=2 * tokens * ff),
        name="step",
    )(x, dy, wg, wu, wd)


def adamw_kernel(count, ssq_ref, gg_ref, gd_ref, *refs):
    ins, outs = refs[:9], refs[9:]
    mean = jnp.sum(ssq_ref[...]) / count
    factor = jnp.minimum(1.0, 0.5 * lax.rsqrt(jnp.full((8, LANES), mean, F32) + 1e-30))[0:1, 0:1]

    def update(which, rows, cols, g):
        at = (0, rows, cols)
        g = g.astype(F32) * factor
        w, m, v = (ins[3 * k + which][at] for k in range(3))
        m = 0.9 * m + 0.1 * g
        v = 0.95 * v + 0.05 * g * g
        w = w.astype(F32)
        outs[which][at] = (w - 0.02 * (m * lax.rsqrt(v + 1e-8) + 0.1 * w)).astype(BF16)
        outs[3 + which][at] = m
        outs[6 + which][at] = v

    every = slice(None)
    tiles = gg_ref.shape[0]
    for t in range(tiles):
        for b in range(4):
            col = LANES * (6 * (t % 4) + 3 * (b % 2) + t // 4)
            update(b // 2, every, slice(col, col + LANES), gg_ref[t, b])
    for ch in range(3):
        update(2, slice(LANES * ch, LANES * ch + LANES), every, gd_ref[0, ch, 0].astype(F32).T)


def run_adamw(count, ssq, gg, gd, arrays):
    layers, rows, ff = arrays[0].shape
    _, drows, d = arrays[2].shape
    tiles = ff // TILE
    parts = 4
    gg = gg.reshape(layers * tiles, 4, LANES, LANES)
    gd = gd.reshape(layers, 3, 4, 256, LANES)
    wide = pl.BlockSpec((1, rows // parts, ff), lambda l, p: (l, p, 0))
    tall = pl.BlockSpec((1, drows, d // parts), lambda l, p: (l, 0, p))
    specs = [wide, wide, tall]
    last = layers - 1
    return pl.pallas_call(
        functools.partial(adamw_kernel, count),
        grid=(layers, parts),
        out_shape=tuple(jax.ShapeDtypeStruct(a.shape, a.dtype) for a in arrays),
        in_specs=[
            pl.BlockSpec((8, LANES), lambda l, p: (0, 0)),
            pl.BlockSpec((tiles, 4, rows // parts, LANES), lambda l, p: (last - l, 0, p, 0)),
            pl.BlockSpec((1, 3, 1, 256, LANES), lambda l, p: (last - l, 0, p, 0, 0)),
        ] + specs * 3,
        out_specs=tuple(specs * 3),
        compiler_params=pltpu.CompilerParams(vmem_limit_bytes=60_000_000),
        name="adamw",
    )(ssq, gg, gd, *arrays)


def solution(mesh):
    n = mesh.shape["dp"]

    def step(x, dy, *arrays):
        gg, gd, ssq = run_step(x, dy, *arrays[:3], n)[:3]
        count = float(n * sum(w.size for w in arrays[:3]))
        return run_adamw(count, ssq, gg, gd, arrays)

    states, cut = P(("rep", "dp"), None, None), P(None, "dp", None)
    return jax.shard_map(
        step,
        mesh=mesh,
        in_specs=(states, states) + (cut,) * 9,
        out_specs=(P("rep", "dp", None),) * 9,
        check_vma=False,
    )
```
